32 devices in a mesh: rows: 8 (over y, x, core), sub: 4 (over z).
Axes of the slice: x: 2, y: 2, z: 4, core: 2. Of those that a mesh axis runs over, the one named last changes fastest.
Arguments:
- u_fem: float32 [120, 524288], P(None, ('rows', 'sub')), may hold values from -600 to 600
- resid_fem: float32 [1, 524288], P(None, ('rows', 'sub')), may hold values from -60 to 60
- slot_map: int32 [32, 32], P(('rows', 'sub')), may hold values from 0 to 31, as said below
- restart: float32 [120, 40], replicated, may hold values from -0.5 to 0.5
- coeff: float32 [3, 120, 120], P(None, None, 'sub'), may hold values from -6 to 6
Outputs:
- new_basis: float32 [40, 524288], P(None, ('rows', 'sub'))
- next_vector: float32 [1, 524288], P(None, ('rows', 'sub'))
- new_coeff: float32 [3, 40, 120], replicated
The draws below stay inside these ranges and needn't reach their ends.
Inputs may be any that keep to these rules, and one draw needn't show every extreme that they name: Each row of slot_map is a permutation of 0 to 31.
All inputs are finite; a program needn't handle non-finite values.
Results may differ from the reference program's by a relative error of at most 0.00015.
Values sent between devices are 32-bit elements; how exact they have to be, the bound alone decides.
No kernel may reach another device: no remote copies, remote signals or barrier semaphores. Data moves between devices by JAX's collectives and lax.ppermute only.
A program may use at most 64 MiB of HBM per device.

```python
import math
import jax
import jax.numpy as jnp
from jax import lax

K = 120
KEEP = 40
DEG = 3
M = 120
NDEV = 32
BS = 512
NROWS = 524288


def basis_core(key):
    core_key = jax.random.fold_in(key, 11)
    core = jnp.clip(jax.random.normal(core_key, (K, NROWS), jnp.float32), -5.0, 5.0)
    position = jnp.arange(NROWS, dtype=jnp.float32) / NROWS
    block_scale = jnp.exp(jax.random.uniform(jax.random.fold_in(key, 12), (NROWS // BS,), jnp.float32, math.log(0.5), math.log(2.0)))
    jitter = jax.random.uniform(jax.random.fold_in(key, 13), (NROWS,), jnp.float32, 0.7, 1.3)
    row_scale = (1.0 + 2.0 * position) * jnp.repeat(block_scale, BS) * jitter
    return (core, row_scale)


def draw_u_fem(key, part):
    core, row_scale = basis_core(key)
    width_scale = jnp.exp(jax.random.uniform(jax.random.fold_in(key, 21), (K,), jnp.float32, 0.0, math.log(10.0)))
    mixing = jnp.eye(K, dtype=jnp.float32) + 0.25 * jax.random.normal(jax.random.fold_in(key, 22), (K, K), jnp.float32) / math.sqrt(K)
    mixed = jnp.dot(mixing, core, precision=lax.Precision.HIGHEST)
    values = width_scale[:, None] * mixed * row_scale[None, :]
    return jnp.clip(values, -600.0, 600.0).astype(jnp.float32)


def draw_resid_fem(key, part):
    core, row_scale = basis_core(key)
    weights = jax.random.normal(jax.random.fold_in(key, 31), (K,), jnp.float32) / math.sqrt(K)
    noise = jnp.clip(jax.random.normal(jax.random.fold_in(key, 32), (NROWS,), jnp.float32), -5.0, 5.0)
    values = (jnp.dot(weights, core, precision=lax.Precision.HIGHEST) + noise) * row_scale
    return jnp.clip(values, -60.0, 60.0)[None, :].astype(jnp.float32)


def draw_slot_map(key, part):
    row_keys = jax.random.split(jax.random.fold_in(key, 41), NDEV)
    return jax.vmap(lambda one_key: jax.random.permutation(one_key, NDEV))(row_keys).astype(jnp.int32)


def steps_of(own_key, shape, cuts, least, high):
    def one(dim, parts):
        draws = jax.random.uniform(jax.random.fold_in(jax.random.fold_in(own_key, 6), dim), (parts,), jnp.float32, least / len(cuts), high / len(cuts))
        return jnp.repeat(jnp.exp(draws), shape[dim] // parts).reshape((-1,) + (1,) * (len(shape) - dim - 1))

    gain = one(*cuts[0])
    for cut in cuts[1:]:
        gain = gain * one(*cut)
    return gain


def gaussian(rng, extent, spread, limit, cuts=(), kind=jnp.bfloat16):
    result = spread * jax.random.normal(rng, extent, jnp.float32)
    if cuts:
        result = result * steps_of(rng, extent, cuts, -0.22, 0.18)
    return jnp.clip(result, -limit, limit).astype(kind)


def setup_inputs(seed: int = 0) -> dict:
    seeds = jax.random.split(jax.random.key(seed), 6)
    return {
        "u_fem": draw_u_fem(jax.random.fold_in(seeds[5], 71), 0),
        "resid_fem": draw_resid_fem(jax.random.fold_in(seeds[5], 71), 0),
        "slot_map": draw_slot_map(jax.random.fold_in(seeds[5], 71), 0),
        "restart": gaussian(seeds[3], (K, KEEP), K ** -0.5, 0.5, (), jnp.float32),
        "coeff": gaussian(seeds[4], (DEG, K, M), 1.0, 6.0, ((2, 4),), jnp.float32),
    }


def relayout(values, slot_map):
    width = values.shape[0]
    blocks = values.reshape(width, NDEV, NDEV, BS).transpose(0, 2, 1, 3)
    source = jnp.argsort(slot_map, axis=1).astype(jnp.int32)
    moved = jnp.take_along_axis(blocks, source[None, :, :, None], axis=2)
    return moved.reshape(width, NROWS)

def reference(u_fem, resid_fem, slot_map, restart, coeff):
    highest = lax.Precision.HIGHEST
    gram_sum = jnp.einsum('kn,jn->kj', u_fem, u_fem, precision=highest) / NROWS
    inner_prod = jnp.einsum('kn,n->k', u_fem, resid_fem[0], precision=highest)
    chol_lower = jnp.linalg.cholesky(gram_sum)
    factor = lax.linalg.triangular_solve(chol_lower, restart, left_side=True, lower=True, transpose_a=True)
    new_rows = jnp.einsum('kp,kn->pn', factor, u_fem, precision=highest)
    half_solve = lax.linalg.triangular_solve(chol_lower, inner_prod[:, None], left_side=True, lower=True)
    proj_coef = lax.linalg.triangular_solve(chol_lower, half_solve, left_side=True, lower=True, transpose_a=True)[:, 0] / NROWS
    remainder = resid_fem - jnp.einsum('k,kn->n', proj_coef, u_fem, precision=highest)[None, :]
    norm_sum = jnp.sum(remainder * remainder)
    next_row = remainder * lax.rsqrt(norm_sum / NROWS + 1e-06)
    raised = jnp.dot(chol_lower, restart, precision=highest)
    rotated = jnp.einsum('kp,ikm->ipm', raised, coeff, precision=highest)
    new_coeff = rotated * lax.rsqrt(jnp.mean(rotated * rotated) + 1e-06)
    return (relayout(new_rows, slot_map), relayout(next_row, slot_map), new_coeff)
```

```python
import functools

import jax
import jax.numpy as jnp
from jax import lax
from jax.experimental import pallas as pl
from jax.experimental.pallas import tpu as pltpu
from jax.sharding import PartitionSpec as P

AXES = ("rows", "sub")
LANES = 128
HIGH = lax.Precision.HIGHEST


def split(x):
    hi = x.astype(jnp.bfloat16)
    lo = (x - hi.astype(jnp.float32)).astype(jnp.bfloat16)
    return hi, lo


def augmented(u, r):
    pad = LANES - u.shape[0] - 1
    return jnp.concatenate([u, r, jnp.zeros((pad, u.shape[1]), jnp.float32)], axis=0)


def gram_body(u_ref, r_ref, out_ref, acc_ref):
    step = pl.program_id(0)
    both = jnp.concatenate(split(augmented(u_ref[...], r_ref[...])), axis=0)
    part = lax.dot_general(both, both, (((1,), (1,)), ((), ())), preferred_element_type=jnp.float32)

    @pl.when(step == 0)
    def _():
        acc_ref[...] = part

    @pl.when(step > 0)
    def _():
        acc_ref[...] += part

    @pl.when(step == pl.num_programs(0) - 1)
    def _():
        acc = acc_ref[...]
        out_ref[...] = (acc[:LANES, :LANES] + acc[LANES:, LANES:]) + (acc[:LANES, LANES:] + acc[LANES:, :LANES])


def gram_call(u, r, tile):
    k, n = u.shape
    return pl.pallas_call(
        gram_body,
        grid=(n // tile,),
        in_specs=[pl.BlockSpec((k, tile), lambda i: (0, i)), pl.BlockSpec((1, tile), lambda i: (0, i))],
        out_specs=pl.BlockSpec((LANES, LANES), lambda i: (0, 0)),
        out_shape=jax.ShapeDtypeStruct((LANES, LANES), jnp.float32),
        scratch_shapes=[pltpu.VMEM((2 * LANES, 2 * LANES), jnp.float32)],
        name="gram",
    )(u, r)


def dot_t(a, b):
    return lax.dot_general(a, b, (((0,), (0,)), ((), ())), precision=HIGH, preferred_element_type=jnp.float32)


def factor_body(s_ref, restart_ref, w_ref, raised_ref, *, k, nrows):
    keep = restart_ref.shape[1]
    row = lax.broadcasted_iota(jnp.int32, (LANES, LANES), 0)
    col = lax.broadcasted_iota(jnp.int32, (LANES, LANES), 1)
    s = s_ref[...]
    a = jnp.where((row < k) & (col < k), s * (1.0 / nrows), 0.0)
    inv = jnp.where(row == col, 1.0, 0.0).astype(jnp.float32)
    inner = s[k : k + 1, :] * (1.0 / nrows)
    low_t = []
    low_i = []
    for i in range(k):
        base = (i // 8) * 8
        off = i - i // 8 * 8
        pivot = a[off : off + 1, i : i + 1]
        scale = lax.rsqrt(pivot)
        scale = scale * (1.5 - 0.5 * pivot * scale * scale)
        urow = a[off : off + 1, :] * scale
        irow = inv[off : off + 1, :] * scale
        low_t.append(urow)
        low_i.append(irow)
        coef = a[:, i : i + 1] * scale
        a = a - coef * urow
        inv = inv - coef * irow
        if off == 7:
            a = a[8:, :]
            inv = inv[8:, :]
    zero = jnp.zeros((LANES - k, LANES), jnp.float32)
    low_t = jnp.concatenate(low_t + [zero], axis=0)
    low_i = jnp.concatenate(low_i + [zero], axis=0)
    low_t = jnp.where(col >= row, low_t, 0.0)
    low_i = jnp.where(col <= row, low_i, 0.0)
    restart = jnp.concatenate([restart_ref[...], jnp.zeros((LANES - k, keep), jnp.float32)], axis=0)
    factor_t = dot_t(restart, low_i)
    raised_ref[...] = dot_t(low_t, restart)
    half = jnp.sum(low_i * inner, axis=1, keepdims=True)
    proj = jnp.sum(low_i * half, axis=0, keepdims=True)
    lane = lax.broadcasted_iota(jnp.int32, (1, LANES), 1)
    last = jnp.where(lane < k, -proj, jnp.where(lane == k, 1.0, 0.0))
    pad = w_ref.shape[0] - keep - 1
    w_ref[...] = jnp.concatenate([factor_t, last, jnp.zeros((pad, LANES), jnp.float32)], axis=0)


def factor_call(s, restart, nrows, wrows):
    k, keep = restart.shape
    return pl.pallas_call(
        functools.partial(factor_body, k=k, nrows=nrows),
        out_shape=(
            jax.ShapeDtypeStruct((wrows, LANES), jnp.float32),
            jax.ShapeDtypeStruct((LANES, keep), jnp.float32),
        ),
        name="factor",
    )(s, restart)


def project_body(u_ref, r_ref, w_ref, out_ref, sum_ref, *, keep, block):
    step = pl.program_id(0)
    tile = u_ref.shape[1]
    per = tile // block
    chunks = block // LANES
    x = jnp.concatenate(split(augmented(u_ref[...], r_ref[...])), axis=0)
    whi, wlo = split(w_ref[...])
    w = jnp.concatenate([jnp.concatenate([whi, whi], axis=1), jnp.concatenate([wlo, wlo], axis=1)], axis=0)
    y = lax.dot_general(w, x, (((1,), (0,)), ((), ())), preferred_element_type=jnp.float32)
    half = w_ref.shape[0]
    y = y[:half] + y[half:]
    total = jnp.zeros((1, LANES), jnp.float32)
    for b in range(per):
        for c in range(chunks):
            lo = b * block + c * LANES
            out_ref[step * per + b, c * keep : (c + 1) * keep, :] = y[:keep, lo : lo + LANES]
            tail = y[keep : keep + 1, lo : lo + LANES]
            out_ref[step * per + b, chunks * keep + c : chunks * keep + c + 1, :] = tail
            total = total + tail * tail

    @pl.when(step == 0)
    def _():
        sum_ref[...] = total

    @pl.when(step > 0)
    def _():
        sum_ref[...] += total

    @pl.when(step == pl.num_programs(0) - 1)
    def _():
        first = chunks * (keep + 1)
        rest = out_ref.shape[1] - first
        out_ref[:, first:, :] = jnp.broadcast_to(sum_ref[...][None], (out_ref.shape[0], rest, LANES))


def project_call(u, r, w, ndev, keep, block, height, tile):
    k, n = u.shape
    return pl.pallas_call(
        functools.partial(project_body, keep=keep, block=block),
        grid=(n // tile,),
        in_specs=[
            pl.BlockSpec((k, tile), lambda i: (0, i)),
            pl.BlockSpec((1, tile), lambda i: (0, i)),
            pl.BlockSpec(w.shape, lambda i: (0, 0)),
        ],
        out_specs=pl.BlockSpec((ndev, height, LANES), lambda i: (0, 0, 0)),
        out_shape=jax.ShapeDtypeStruct((ndev, height, LANES), jnp.float32),
        scratch_shapes=[pltpu.VMEM((1, LANES), jnp.float32)],
        name="project",
    )(u, r, w)


def settle_body(slot_ref, got_ref, rows_ref, next_ref, *, keep, block, nrows):
    ndev = got_ref.shape[0]
    chunks = block // LANES
    first = chunks * (keep + 1)
    total = jnp.sum(got_ref[:, first, :])
    scale = lax.rsqrt(jnp.full((1, LANES), total / nrows + 1e-06, jnp.float32))

    def move(d, carry):
        start = pl.multiple_of(slot_ref[0, d] * block, block)
        for c in range(chunks):
            rows_ref[:, pl.ds(start + c * LANES, LANES)] = got_ref[d, c * keep : (c + 1) * keep, :]
            tail = got_ref[d, chunks * keep + c : chunks * keep + c + 1, :]
            next_ref[:, pl.ds(start + c * LANES, LANES)] = tail * scale
        return carry

    lax.fori_loop(0, ndev, move, 0)


def settle_call(slots, got, keep, block, nrows):
    n = got.shape[0] * block
    return pl.pallas_call(
        functools.partial(settle_body, keep=keep, block=block, nrows=nrows),
        in_specs=[pl.BlockSpec(memory_space=pltpu.SMEM), pl.BlockSpec(memory_space=pltpu.VMEM)],
        out_shape=(jax.ShapeDtypeStruct((keep, n), jnp.float32), jax.ShapeDtypeStruct((1, n), jnp.float32)),
        name="settle",
    )(slots, got)


def local(u_fem, resid_fem, slot_map, restart, coeff):
    ndev = lax.axis_size(AXES)
    nsub = lax.axis_size("sub")
    k, n = u_fem.shape
    keep = restart.shape[1]
    nrows = n * ndev
    block = n // ndev
    chunks = block // LANES
    tile = block * max(1, min(ndev, 2048 // block))

    coeff_all = lax.all_to_all(jnp.broadcast_to(coeff[None], (nsub,) + coeff.shape), "sub", 0, 0, tiled=True)
    gram = gram_call(u_fem, resid_fem, tile)
    per = -(-LANES // ndev)
    gram = jnp.pad(gram, ((0, per * ndev - LANES), (0, 0))).reshape(ndev, per, LANES)
    part = lax.all_to_all(gram, AXES, 0, 0, tiled=True).sum(axis=0, keepdims=True)
    whole = lax.all_to_all(jnp.broadcast_to(part, (ndev, per, LANES)), AXES, 0, 0, tiled=True)
    whole = whole.reshape(ndev * per, LANES)[:LANES]

    wrows = -(-(keep + 1) // 8) * 8
    w, raised = factor_call(whole, restart, float(nrows), wrows)
    height = -(-(chunks * (keep + 1) + 1) // 8) * 8
    sent = project_call(u_fem, resid_fem, w, ndev, keep, block, height, tile)
    got = lax.all_to_all(sent, AXES, 0, 0, tiled=True)
    new_rows, next_row = settle_call(slot_map, got, keep, block, float(nrows))

    coeff_all = jnp.moveaxis(coeff_all, 0, 2).reshape(coeff.shape[0], k, -1)
    rotated = jnp.einsum("kp,ikm->ipm", raised[:k], coeff_all, precision=HIGH)
    new_coeff = rotated * lax.rsqrt(jnp.mean(rotated * rotated) + 1e-06)
    return (new_rows, next_row, new_coeff)


def solution(mesh):
    in_specs = (
        P(None, AXES),
        P(None, AXES),
        P(AXES, None),
        P(),
        P(None, None, "sub"),
    )
    out_specs = (P(None, AXES), P(None, AXES), P())
    return jax.shard_map(local, mesh=mesh, in_specs=in_specs, out_specs=out_specs, check_vma=False)
```

```python
import functools

import jax
import jax.numpy as jnp
from jax import lax
from jax.experimental import pallas as pl
from jax.experimental.pallas import tpu as pltpu
from jax.sharding import PartitionSpec as P

AXES = ("rows", "sub")
LANES = 128
HIGH = lax.Precision.HIGHEST


def split(x):
    hi = x.astype(jnp.bfloat16)
    lo = (x - hi.astype(jnp.float32)).astype(jnp.bfloat16)
    return hi, lo


def augmented(u, r):
    pad = LANES - u.shape[0] - 1
    return jnp.concatenate([u, r, jnp.zeros((pad, u.shape[1]), jnp.float32)], axis=0)


def gram_body(u_hbm, r_hbm, out_ref, u_ref, r_ref, sems, *, tile):
    k, n = u_hbm.shape
    steps = n // tile

    def copy(i):
        cut = pl.ds(i * tile, tile)
        return pltpu.make_async_copy(u_hbm.at[:, cut], u_ref.at[:, cut], sems.at[i])

    rows = pltpu.make_async_copy(r_hbm, r_ref, sems.at[steps])
    rows.start()
    for i in range(steps):
        copy(i).start()
    rows.wait()
    acc = jnp.zeros((2 * LANES, 2 * LANES), jnp.float32)
    for i in range(steps):
        copy(i).wait()
        cut = pl.ds(i * tile, tile)
        both = jnp.concatenate(split(augmented(u_ref[:, cut], r_ref[:, cut])), axis=0)
        acc = acc + lax.dot_general(both, both, (((1,), (1,)), ((), ())), preferred_element_type=jnp.float32)
    out_ref[...] = (acc[:LANES, :LANES] + acc[LANES:, LANES:]) + (acc[:LANES, LANES:] + acc[LANES:, :LANES])


def gram_call(u, r, tile):
    k, n = u.shape
    far = pl.BlockSpec(memory_space=pltpu.HBM)
    return pl.pallas_call(
        functools.partial(gram_body, tile=tile),
        in_specs=[far, far],
        out_specs=pl.BlockSpec(memory_space=pltpu.VMEM),
        out_shape=pltpu.VMEM((LANES, LANES), jnp.float32),
        scratch_shapes=[
            pltpu.VMEM((k, n), jnp.float32),
            pltpu.VMEM((1, n), jnp.float32),
            pltpu.SemaphoreType.DMA((n // tile + 1,)),
        ],
        name="gram",
        compiler_params=pltpu.CompilerParams(vmem_limit_bytes=58 << 20),
    )(u, r)


def dot_t(a, b):
    return lax.dot_general(a, b, (((0,), (0,)), ((), ())), precision=HIGH, preferred_element_type=jnp.float32)


def root(pivot):
    scale = lax.rsqrt(pivot)
    return scale * (1.5 - 0.5 * pivot * scale * scale)


def update_body(
    s_ref, restart_ref, u_hbm, r_hbm, sent_hbm, raised_ref, u_ref, r_ref, sent_ref, in_sems, out_sems, *, nrows, block, tile
):
    k, n = u_hbm.shape
    keep = restart_ref.shape[1]
    steps = n // tile
    per = tile // block
    chunks = block // LANES
    body = chunks * keep

    def fetch(i):
        cut = pl.ds(i * tile, tile)
        return pltpu.make_async_copy(u_hbm.at[:, cut], u_ref.at[:, cut], in_sems.at[i])

    def ship(i):
        at = (pl.ds(i * per, per), pl.ds(0, body))
        return pltpu.make_async_copy(sent_ref.at[at], sent_hbm.at[at], out_sems.at[i])

    rows = pltpu.make_async_copy(r_hbm, r_ref, in_sems.at[steps])
    rows.start()
    for i in range(steps):
        fetch(i).start()
    row = lax.broadcasted_iota(jnp.int32, (LANES, LANES), 0)
    col = lax.broadcasted_iota(jnp.int32, (LANES, LANES), 1)
    s = s_ref[...]
    a = jnp.where((row < k) & (col < k), s * (1.0 / nrows), 0.0)
    inv = jnp.where(row == col, 1.0, 0.0).astype(jnp.float32)
    inner = s[k : k + 1, :] * (1.0 / nrows)
    low_t = []
    low_i = []
    for i in range(0, k, 2):
        off = i % 8
        col0 = jnp.broadcast_to(a[:, i : i + 1], a.shape)
        col1 = jnp.broadcast_to(a[:, i + 1 : i + 2], a.shape)
        scale0 = root(col0[off : off + 1])
        edge = col0[off + 1 : off + 2] * scale0
        scale1 = root(col1[off + 1 : off + 2] - edge * edge)
        urow0 = a[off : off + 1] * scale0
        urow1 = (a[off + 1 : off + 2] - edge * urow0) * scale1
        irow0 = inv[off : off + 1] * scale0
        irow1 = (inv[off + 1 : off + 2] - edge * irow0) * scale1
        low_t += [urow0, urow1]
        low_i += [irow0, irow1]
        col0 = col0 * scale0
        col1 = (col1 - col0 * edge) * scale1
        a = a - col0 * urow0 - col1 * urow1
        inv = inv - col0 * irow0 - col1 * irow1
        if off == 6:
            a = a[8:]
            inv = inv[8:]
    zero = jnp.zeros((LANES - k, LANES), jnp.float32)
    low_t = jnp.concatenate(low_t + [zero], axis=0)
    low_i = jnp.concatenate(low_i + [zero], axis=0)
    low_t = jnp.where(col >= row, low_t, 0.0)
    low_i = jnp.where(col <= row, low_i, 0.0)
    restart = jnp.concatenate([restart_ref[...], jnp.zeros((LANES - k, keep), jnp.float32)], axis=0)
    factor_t = dot_t(restart, low_i)
    raised_ref[...] = dot_t(low_t, restart)
    half = jnp.sum(low_i * inner, axis=1, keepdims=True)
    proj = jnp.sum(low_i * half, axis=0, keepdims=True)
    lane = lax.broadcasted_iota(jnp.int32, (1, LANES), 1)
    last = jnp.where(lane < k, -proj, jnp.where(lane == k, 1.0, 0.0))
    half = -(-(keep + 1) // 8) * 8
    pad = half - keep - 1
    w = jnp.concatenate([factor_t, last, jnp.zeros((pad, LANES), jnp.float32)], axis=0)
    whi, wlo = split(w)
    w = jnp.concatenate([jnp.concatenate([whi, whi], axis=1), jnp.concatenate([wlo, wlo], axis=1)], axis=0)

    rows.wait()
    total = jnp.zeros((1, LANES), jnp.float32)
    for i in range(steps):
        fetch(i).wait()
        cut = pl.ds(i * tile, tile)
        x = jnp.concatenate(split(augmented(u_ref[:, cut], r_ref[:, cut])), axis=0)
        y = lax.dot_general(w, x, (((1,), (0,)), ((), ())), preferred_element_type=jnp.float32)
        y = y[:half] + y[half:]
        for b in range(per):
            for c in range(chunks):
                lo = b * block + c * LANES
                sent_ref[i * per + b, c * keep : (c + 1) * keep, :] = y[:keep, lo : lo + LANES]
                tail = y[keep : keep + 1, lo : lo + LANES]
                sent_ref[i * per + b, body + c : body + c + 1, :] = tail
                total = total + tail * tail
        ship(i).start()
    first = body + chunks
    rest = sent_ref.shape[1] - first
    sent_ref[:, first:, :] = jnp.broadcast_to(total[None], (sent_ref.shape[0], rest, LANES))
    tails = pltpu.make_async_copy(sent_ref.at[:, body:, :], sent_hbm.at[:, body:, :], out_sems.at[steps])
    tails.start()
    for i in range(steps):
        ship(i).wait()
    tails.wait()


def update_call(s, restart, u, r, ndev, nrows, block, height, tile):
    k, keep = restart.shape
    n = u.shape[1]
    near = pl.BlockSpec(memory_space=pltpu.VMEM)
    far = pl.BlockSpec(memory_space=pltpu.HBM)
    return pl.pallas_call(
        functools.partial(update_body, nrows=nrows, block=block, tile=tile),
        in_specs=[near, near, far, far],
        out_specs=(far, near),
        out_shape=(pltpu.HBM((ndev, height, LANES), jnp.float32), pltpu.VMEM((LANES, keep), jnp.float32)),
        scratch_shapes=[
            pltpu.VMEM((k, n), jnp.float32),
            pltpu.VMEM((1, n), jnp.float32),
            pltpu.VMEM((ndev, height, LANES), jnp.float32),
            pltpu.SemaphoreType.DMA((n // tile + 1,)),
            pltpu.SemaphoreType.DMA((n // tile + 1,)),
        ],
        compiler_params=pltpu.CompilerParams(vmem_limit_bytes=58 << 20),
        name="update",
    )(s, restart, u, r)


def settle_body(slot_ref, got_ref, rows_ref, next_ref, tail_ref, sems, *, keep, block, nrows):
    ndev = got_ref.shape[0]
    chunks = block // LANES
    tails = pltpu.make_async_copy(got_ref.at[:, chunks * keep :, :], tail_ref, sems.at[0])
    tails.start()

    def move(d, carry):
        start = pl.multiple_of(slot_ref[0, d] * block, block)
        for c in range(chunks):
            pltpu.make_async_copy(
                got_ref.at[d, c * keep : (c + 1) * keep, :], rows_ref.at[:, pl.ds(start + c * LANES, LANES)], sems.at[1]
            ).start()
        return carry

    lax.fori_loop(0, ndev, move, 0)
    tails.wait()
    total = jnp.sum(tail_ref[:, chunks, :])
    scale = lax.rsqrt(jnp.full((1, LANES), total / nrows + 1e-06, jnp.float32))

    def place(d, carry):
        start = pl.multiple_of(slot_ref[0, d] * block, block)
        for c in range(chunks):
            next_ref[:, pl.ds(start + c * LANES, LANES)] = tail_ref[d, c : c + 1, :] * scale
        return carry

    lax.fori_loop(0, ndev, place, 0)
    pltpu.make_async_copy(rows_ref, rows_ref, sems.at[1]).wait()


def settle_call(slots, got, keep, block, nrows):
    ndev, height, _ = got.shape
    n = ndev * block
    chunks = block // LANES
    anywhere = pl.BlockSpec(memory_space=pl.ANY)
    return pl.pallas_call(
        functools.partial(settle_body, keep=keep, block=block, nrows=nrows),
        in_specs=[pl.BlockSpec(memory_space=pltpu.SMEM), anywhere],
        out_specs=(anywhere, pl.BlockSpec(memory_space=pltpu.VMEM)),
        out_shape=(jax.ShapeDtypeStruct((keep, n), jnp.float32), jax.ShapeDtypeStruct((1, n), jnp.float32)),
        scratch_shapes=[
            pltpu.VMEM((ndev, height - chunks * keep, LANES), jnp.float32),
            pltpu.SemaphoreType.DMA((2,)),
        ],
        name="settle",
        compiler_params=pltpu.CompilerParams(vmem_limit_bytes=12 << 20),
    )(slots, got)


def total_of(x, ndev):
    if ndev & (ndev - 1):
        return lax.psum(x, AXES)
    bit = 1
    while bit < ndev:
        x = x + lax.ppermute(x, AXES, [(i, i ^ bit) for i in range(ndev)])
        bit *= 2
    return x


def gather_sub(x):
    nsub = lax.axis_size("sub")
    turns = [x] + [lax.ppermute(x, "sub", [(i, (i + d) % nsub) for i in range(nsub)]) for d in range(1, nsub)]
    order = (lax.axis_index("sub") - jnp.arange(nsub)) % nsub
    picks = jax.nn.one_hot(order, nsub, dtype=jnp.bool_)
    return jnp.stack(
        [functools.reduce(lambda a, b: a + b, [jnp.where(picks[t, d], turns[d], 0.0) for d in range(nsub)]) for t in range(nsub)]
    )


def local(u_fem, resid_fem, slot_map, restart, coeff):
    ndev = lax.axis_size(AXES)
    k, n = u_fem.shape
    keep = restart.shape[1]
    nrows = n * ndev
    block = n // ndev
    chunks = block // LANES
    tile = block * max(1, min(ndev, 2048 // block))

    whole = total_of(gram_call(u_fem, resid_fem, tile), ndev)
    height = -(-(chunks * (keep + 1) + 1) // 8) * 8
    sent, raised = update_call(whole, restart, u_fem, resid_fem, ndev, float(nrows), block, height, tile)
    got = lax.all_to_all(sent, AXES, 0, 0, tiled=True)
    new_rows, next_row = settle_call(slot_map, got, keep, block, float(nrows))

    rotated = jnp.einsum("kp,ikm->ipm", raised[:k], coeff, precision=HIGH)
    rotated = jnp.moveaxis(gather_sub(rotated), 0, 2).reshape(coeff.shape[0], keep, -1)
    new_coeff = rotated * lax.rsqrt(jnp.mean(rotated * rotated) + 1e-06)
    return (new_rows, next_row, new_coeff)


def solution(mesh):
    in_specs = (
        P(None, AXES),
        P(None, AXES),
        P(AXES, None),
        P(),
        P(None, None, "sub"),
    )
    out_specs = (P(None, AXES), P(None, AXES), P())
    return jax.shard_map(local, mesh=mesh, in_specs=in_specs, out_specs=out_specs, check_vma=False)
```

```python
import functools

import jax
import jax.numpy as jnp
from jax import lax
from jax.experimental import pallas as pl
from jax.experimental.pallas import tpu as pltpu
from jax.sharding import PartitionSpec as P

AXES = ("rows", "sub")
LANES = 128
HIGH = lax.Precision.HIGHEST


def split(x):
    hi = x.astype(jnp.bfloat16)
    lo = (x - hi.astype(jnp.float32)).astype(jnp.bfloat16)
    return hi, lo


def augmented(u, r):
    pad = LANES - u.shape[0] - 1
    return jnp.concatenate([u, r, jnp.zeros((pad, u.shape[1]), jnp.float32)], axis=0)


def gram_body(u_hbm, r_hbm, out_ref, u_ref, r_ref, sems, *, tile):
    k, n = u_hbm.shape
    steps = n // tile

    def copy(i):
        cut = pl.ds(i * tile, tile)
        return pltpu.make_async_copy(u_hbm.at[:, cut], u_ref.at[:, cut], sems.at[i])

    rows = pltpu.make_async_copy(r_hbm, r_ref, sems.at[steps])
    rows.start()
    for i in range(steps):
        copy(i).start()
    rows.wait()
    acc = jnp.zeros((2 * LANES, 2 * LANES), jnp.float32)
    for i in range(steps):
        copy(i).wait()
        cut = pl.ds(i * tile, tile)
        both = jnp.concatenate(split(augmented(u_ref[:, cut], r_ref[:, cut])), axis=0)
        acc = acc + lax.dot_general(both, both, (((1,), (1,)), ((), ())), preferred_element_type=jnp.float32)
    out_ref[...] = (acc[:LANES, :LANES] + acc[LANES:, LANES:]) + (acc[:LANES, LANES:] + acc[LANES:, :LANES])


def gram_call(u, r, tile):
    k, n = u.shape
    far = pl.BlockSpec(memory_space=pltpu.HBM)
    return pl.pallas_call(
        functools.partial(gram_body, tile=tile),
        in_specs=[far, far],
        out_specs=pl.BlockSpec(memory_space=pltpu.VMEM),
        out_shape=pltpu.VMEM((LANES, LANES), jnp.float32),
        scratch_shapes=[
            pltpu.VMEM((k, n), jnp.float32),
            pltpu.VMEM((1, n), jnp.float32),
            pltpu.SemaphoreType.DMA((n // tile + 1,)),
        ],
        name="gram",
        compiler_params=pltpu.CompilerParams(vmem_limit_bytes=58 << 20),
    )(u, r)


def dot_t(a, b):
    return lax.dot_general(a, b, (((0,), (0,)), ((), ())), precision=HIGH, preferred_element_type=jnp.float32)


def root(pivot):
    scale = lax.rsqrt(pivot)
    return scale * (1.5 - 0.5 * pivot * scale * scale)


def update_body(
    s_ref, restart_ref, u_hbm, r_hbm, sent_hbm, raised_ref, u_ref, r_ref, sent_ref, in_sems, out_sems, *, nrows, block, tile
):
    k, n = u_hbm.shape
    keep = restart_ref.shape[1]
    steps = n // tile
    per = tile // block
    chunks = block // LANES
    body = chunks * keep

    def fetch(i):
        cut = pl.ds(i * tile, tile)
        return pltpu.make_async_copy(u_hbm.at[:, cut], u_ref.at[:, cut], in_sems.at[i])

    def ship(i):
        at = (pl.ds(i * per, per), pl.ds(0, body))
        return pltpu.make_async_copy(sent_ref.at[at], sent_hbm.at[at], out_sems.at[i])

    rows = pltpu.make_async_copy(r_hbm, r_ref, in_sems.at[steps])
    rows.start()
    for i in range(steps):
        fetch(i).start()
    row = lax.broadcasted_iota(jnp.int32, (LANES, LANES), 0)
    col = lax.broadcasted_iota(jnp.int32, (LANES, LANES), 1)
    s = s_ref[...]
    a = jnp.where((row < k) & (col < k), s * (1.0 / nrows), 0.0)
    inv = jnp.where(row == col, 1.0, 0.0).astype(jnp.float32)
    inner = s[k : k + 1, :] * (1.0 / nrows)
    low_t = []
    low_i = []
    for i in range(0, k, 2):
        off = i % 8
        col0 = jnp.broadcast_to(a[:, i : i + 1], a.shape)
        col1 = jnp.broadcast_to(a[:, i + 1 : i + 2], a.shape)
        scale0 = root(col0[off : off + 1])
        edge = col0[off + 1 : off + 2] * scale0
        scale1 = root(col1[off + 1 : off + 2] - edge * edge)
        urow0 = a[off : off + 1] * scale0
        urow1 = (a[off + 1 : off + 2] - edge * urow0) * scale1
        irow0 = inv[off : off + 1] * scale0
        irow1 = (inv[off + 1 : off + 2] - edge * irow0) * scale1
        low_t += [urow0, urow1]
        low_i += [irow0, irow1]
        col0 = col0 * scale0
        col1 = (col1 - col0 * edge) * scale1
        a = a - col0 * urow0 - col1 * urow1
        inv = inv - col0 * irow0 - col1 * irow1
        if off == 6:
            a = a[8:]
            inv = inv[8:]
    zero = jnp.zeros((LANES - k, LANES), jnp.float32)
    low_t = jnp.concatenate(low_t + [zero], axis=0)
    low_i = jnp.concatenate(low_i + [zero], axis=0)
    low_t = jnp.where(col >= row, low_t, 0.0)
    low_i = jnp.where(col <= row, low_i, 0.0)
    restart = jnp.concatenate([restart_ref[...], jnp.zeros((LANES - k, keep), jnp.float32)], axis=0)
    factor_t = dot_t(restart, low_i)
    raised_ref[...] = dot_t(low_t, restart)
    half = jnp.sum(low_i * inner, axis=1, keepdims=True)
    proj = jnp.sum(low_i * half, axis=0, keepdims=True)
    lane = lax.broadcasted_iota(jnp.int32, (1, LANES), 1)
    last = jnp.where(lane < k, -proj, jnp.where(lane == k, 1.0, 0.0))
    half = -(-(keep + 1) // 8) * 8
    pad = half - keep - 1
    w = jnp.concatenate([factor_t, last, jnp.zeros((pad, LANES), jnp.float32)], axis=0)
    whi, wlo = split(w)
    w = jnp.concatenate([jnp.concatenate([whi, whi], axis=1), jnp.concatenate([wlo, wlo], axis=1)], axis=0)

    rows.wait()
    total = jnp.zeros((1, LANES), jnp.float32)
    for i in range(steps):
        fetch(i).wait()
        cut = pl.ds(i * tile, tile)
        x = jnp.concatenate(split(augmented(u_ref[:, cut], r_ref[:, cut])), axis=0)
        y = lax.dot_general(w, x, (((1,), (0,)), ((), ())), preferred_element_type=jnp.float32)
        y = y[:half] + y[half:]
        for b in range(per):
            for c in range(chunks):
                lo = b * block + c * LANES
                sent_ref[i * per + b, c * keep : (c + 1) * keep, :] = y[:keep, lo : lo + LANES]
                tail = y[keep : keep + 1, lo : lo + LANES]
                sent_ref[i * per + b, body + c : body + c + 1, :] = tail
                total = total + tail * tail
        ship(i).start()
    first = body + chunks
    rest = sent_ref.shape[1] - first
    sent_ref[:, first:, :] = jnp.broadcast_to(total[None], (sent_ref.shape[0], rest, LANES))
    tails = pltpu.make_async_copy(sent_ref.at[:, body:, :], sent_hbm.at[:, body:, :], out_sems.at[steps])
    tails.start()
    for i in range(steps):
        ship(i).wait()
    tails.wait()


def update_call(s, restart, u, r, ndev, nrows, block, height, tile):
    k, keep = restart.shape
    n = u.shape[1]
    near = pl.BlockSpec(memory_space=pltpu.VMEM)
    far = pl.BlockSpec(memory_space=pltpu.HBM)
    return pl.pallas_call(
        functools.partial(update_body, nrows=nrows, block=block, tile=tile),
        in_specs=[near, near, far, far],
        out_specs=(far, near),
        out_shape=(pltpu.HBM((ndev, height, LANES), jnp.float32), pltpu.VMEM((LANES, keep), jnp.float32)),
        scratch_shapes=[
            pltpu.VMEM((k, n), jnp.float32),
            pltpu.VMEM((1, n), jnp.float32),
            pltpu.VMEM((ndev, height, LANES), jnp.float32),
            pltpu.SemaphoreType.DMA((n // tile + 1,)),
            pltpu.SemaphoreType.DMA((n // tile + 1,)),
        ],
        compiler_params=pltpu.CompilerParams(vmem_limit_bytes=58 << 20),
        name="update",
    )(s, restart, u, r)


def settle_body(slot_ref, got_ref, rows_ref, next_ref, tail_ref, sems, *, keep, block, nrows):
    ndev = got_ref.shape[0]
    chunks = block // LANES
    tails = pltpu.make_async_copy(got_ref.at[:, chunks * keep :, :], tail_ref, sems.at[0])
    tails.start()

    def move(d, carry):
        start = pl.multiple_of(slot_ref[0, d] * block, block)
        for c in range(chunks):
            pltpu.make_async_copy(
                got_ref.at[d, c * keep : (c + 1) * keep, :], rows_ref.at[:, pl.ds(start + c * LANES, LANES)], sems.at[1]
            ).start()
        return carry

    lax.fori_loop(0, ndev, move, 0)
    tails.wait()
    total = jnp.sum(tail_ref[:, chunks, :])
    scale = lax.rsqrt(jnp.full((1, LANES), total / nrows + 1e-06, jnp.float32))

    def place(d, carry):
        start = pl.multiple_of(slot_ref[0, d] * block, block)
        for c in range(chunks):
            next_ref[:, pl.ds(start + c * LANES, LANES)] = tail_ref[d, c : c + 1, :] * scale
        return carry

    lax.fori_loop(0, ndev, place, 0)
    pltpu.make_async_copy(rows_ref, rows_ref, sems.at[1]).wait()


def settle_call(slots, got, keep, block, nrows):
    ndev, height, _ = got.shape
    n = ndev * block
    chunks = block // LANES
    anywhere = pl.BlockSpec(memory_space=pl.ANY)
    return pl.pallas_call(
        functools.partial(settle_body, keep=keep, block=block, nrows=nrows),
        in_specs=[pl.BlockSpec(memory_space=pltpu.SMEM), anywhere],
        out_specs=(anywhere, pl.BlockSpec(memory_space=pltpu.VMEM)),
        out_shape=(jax.ShapeDtypeStruct((keep, n), jnp.float32), jax.ShapeDtypeStruct((1, n), jnp.float32)),
        scratch_shapes=[
            pltpu.VMEM((ndev, height - chunks * keep, LANES), jnp.float32),
            pltpu.SemaphoreType.DMA((2,)),
        ],
        name="settle",
        compiler_params=pltpu.CompilerParams(vmem_limit_bytes=12 << 20),
    )(slots, got)


def total_of(x, ndev):
    if ndev & (ndev - 1):
        return lax.psum(x, AXES)
    bit = 1
    while bit < ndev:
        x = x + lax.ppermute(x, AXES, [(i, i ^ bit) for i in range(ndev)])
        bit *= 2
    return x


def local(u_fem, resid_fem, slot_map, restart, coeff):
    ndev = lax.axis_size(AXES)
    k, n = u_fem.shape
    keep = restart.shape[1]
    nrows = n * ndev
    block = n // ndev
    chunks = block // LANES
    tile = block * max(1, min(ndev, 2048 // block))

    nsub = lax.axis_size("sub")
    coeff_all = lax.all_to_all(jnp.broadcast_to(coeff[None], (nsub,) + coeff.shape), "sub", 0, 0, tiled=True)
    whole = total_of(gram_call(u_fem, resid_fem, tile), ndev)
    height = -(-(chunks * (keep + 1) + 1) // 8) * 8
    sent, raised = update_call(whole, restart, u_fem, resid_fem, ndev, float(nrows), block, height, tile)
    got = lax.all_to_all(sent, AXES, 0, 0, tiled=True)
    new_rows, next_row = settle_call(slot_map, got, keep, block, float(nrows))

    coeff_all = jnp.moveaxis(coeff_all, 0, 2).reshape(coeff.shape[0], k, -1)
    rotated = jnp.einsum("kp,ikm->ipm", raised[:k], coeff_all, precision=HIGH)
    new_coeff = rotated * lax.rsqrt(jnp.mean(rotated * rotated) + 1e-06)
    return (new_rows, next_row, new_coeff)


def solution(mesh):
    in_specs = (
        P(None, AXES),
        P(None, AXES),
        P(AXES, None),
        P(),
        P(None, None, "sub"),
    )
    out_specs = (P(None, AXES), P(None, AXES), P())
    return jax.shard_map(local, mesh=mesh, in_specs=in_specs, out_specs=out_specs, check_vma=False)
```
